8 devices in a mesh: dp: 1 (over z), ep: 8 (over x, y, core).
Axes of the slice: x: 2, y: 2, z: 1, core: 2. Of those that a mesh axis runs over, the one named last changes fastest.
Arguments:
- x: bfloat16 [1, 8, 256, 4096], P('dp', 'ep')
- expert: int32 [1, 8, 256, 8], P('dp', 'ep')
- slot: int32 [1, 8, 256, 8], P('dp', 'ep')
- gate: float32 [1, 8, 256, 8], P('dp', 'ep')
- w_gate: bfloat16 [64, 4096, 1536], P('ep')
- w_up: bfloat16 [64, 4096, 1536], P('ep')
- w_down: bfloat16 [64, 1536, 4096], P('ep')
Outputs:
- y: bfloat16 [1, 8, 256, 4096], P('dp', 'ep')
All inputs are finite; a program needn't handle non-finite values.
Results may differ from the reference program's by a relative error of at most 0.009.
Values are sent between devices in bfloat16 or wider.
A program may use at most 2 GiB of HBM per device.

```python
import jax
import jax.numpy as jnp

MEMBERS = 8
TOKENS = 256
D = 4096
FF = 1536
TOP = 8
EXPERTS = 64
SLOTS = 5 * TOKENS * TOP // (4 * EXPERTS)


def setup_inputs(seed: int = 0, part: int = 0) -> dict:
    own, k1, k2, k3, k4, k5, k6 = jax.random.split(jax.random.key(seed), 7)
    kx, ke, kl, kg = jax.random.split(jax.random.fold_in(own, part), 4)
    devices = (1, MEMBERS)
    place = jax.random.permutation(kl, jnp.arange(EXPERTS, dtype=jnp.uint32))
    slow = ((EXPERTS + (9 * place) % EXPERTS) << ((9 * place) // EXPERTS)) // EXPERTS
    wait = (jax.random.bits(ke, (*devices, TOKENS, EXPERTS), jnp.uint32) >> 10) * slow
    expert = jnp.argsort(wait, axis=-1)[..., :TOP].astype(jnp.int32)
    chosen = jax.nn.one_hot(expert, EXPERTS, dtype=jnp.int32)
    in_line = jnp.cumsum(chosen.reshape(*devices, TOKENS * TOP, EXPERTS), axis=2) - 1
    slot = jnp.sum(in_line.reshape(chosen.shape) * chosen, axis=-1)

    def one(key, rows, columns):
        return (jax.random.normal(key, (rows, columns), jnp.float32) * rows**-0.5).astype(jnp.bfloat16)

    def weights(key, rows, columns):
        return jax.lax.map(lambda k: one(k, rows, columns), jax.random.split(key, EXPERTS))

    return {
        "x": jax.random.normal(kx, (*devices, TOKENS, D), jnp.float32).astype(jnp.bfloat16),
        "expert": expert,
        "slot": slot,
        "gate": jax.nn.softmax(jax.random.normal(kg, expert.shape, jnp.float32)),
        "w_gate": weights(k1, D, FF),
        "w_up": weights(k2, D, FF),
        "w_down": weights(k3, FF, D),
    }


def einsum(form, a, b):
    return jnp.einsum(form, a.astype(jnp.float32), b.astype(jnp.float32))


def reference(x, expert, slot, gate, w_gate, w_up, w_down):
    to_expert = jax.nn.one_hot(expert, EXPERTS, dtype=jnp.bfloat16)
    to_slot = jax.nn.one_hot(slot, SLOTS, dtype=jnp.bfloat16)
    weighted = to_expert * gate[..., None].astype(jnp.bfloat16)
    dispatch = einsum("abtke,abtkc->abtec", to_expert, to_slot).astype(jnp.bfloat16)
    combine = einsum("abtke,abtkc->abtec", weighted, to_slot).astype(jnp.bfloat16)
    z = einsum("abtec,abtd->aebcd", dispatch, x).astype(jnp.bfloat16)
    h = jax.nn.silu(einsum("aebcd,edf->aebcf", z, w_gate))
    h = (h * einsum("aebcd,edf->aebcf", z, w_up)).astype(jnp.bfloat16)
    out = einsum("aebcf,efd->aebcd", h, w_down).astype(jnp.bfloat16)
    y = einsum("abtec,aebcd->abtd", combine, out)
    return y.astype(jnp.bfloat16)
```

```python
import jax
import jax.numpy as jnp
from jax import lax
from jax.sharding import PartitionSpec as P


def solution(mesh):
    def body(x, expert, slot, gate, w_gate, w_up, w_down):
        tokens, top = expert.shape[2:]
        members = mesh.shape["ep"]
        local, d, ff = w_gate.shape
        slots = 5 * tokens * top // (4 * local * members)
        me = lax.axis_index("ep")

        xs = lax.all_gather(x[0, 0], "ep")
        code = jnp.where(slot[0, 0] < slots, expert[0, 0] * slots + slot[0, 0], -1)
        codes = lax.all_gather(code, "ep") - me * (local * slots)
        gates = lax.all_gather(gate[0, 0], "ep").astype(jnp.bfloat16)
        rows = jnp.arange(local * slots)
        hit = codes[:, None, :, :] == rows[None, :, None, None]
        pick = jnp.any(hit, -1).astype(jnp.bfloat16)
        mix = jnp.sum(jnp.where(hit, gates[:, None], 0), -1, dtype=jnp.float32).astype(jnp.bfloat16)
        z = jnp.einsum("srt,std->srd", pick, xs, preferred_element_type=jnp.float32).astype(jnp.bfloat16)
        z = z.reshape(members, local, slots, d).transpose(1, 0, 2, 3).reshape(local, members * slots, d)
        g = jnp.einsum("emd,edf->emf", z, w_gate, preferred_element_type=jnp.float32)
        u = jnp.einsum("emd,edf->emf", z, w_up, preferred_element_type=jnp.float32)
        h = (jax.nn.silu(g) * u).astype(jnp.bfloat16)
        out = jnp.einsum("emf,efd->emd", h, w_down, preferred_element_type=jnp.float32).astype(jnp.bfloat16)
        out = out.reshape(local, members, slots, d).transpose(1, 0, 2, 3).reshape(members, local * slots, d)
        y = jnp.einsum("srt,srd->std", mix, out, preferred_element_type=jnp.float32).astype(jnp.bfloat16)
        y = lax.psum_scatter(y, "ep", scatter_dimension=0)
        return y[None, None].astype(jnp.bfloat16)

    tok = P("dp", "ep", None, None)
    w = P("ep", None, None)
    return jax.shard_map(
        body, mesh=mesh, in_specs=(tok, tok, tok, tok, w, w, w), out_specs=tok, check_vma=False
    )
```

```python
import functools

import jax
import jax.numpy as jnp
from jax import lax
from jax.experimental import pallas as pl
from jax.experimental.pallas import tpu as pltpu
from jax.sharding import PartitionSpec as P

MESH = pl.DeviceIdType.MESH
F32, BF16 = jnp.float32, jnp.bfloat16
CH = 512
NW = 6
H, T, M, SL, PAD, KP = 128, 256, 320, 40, 48, 384
PAIR, PT, LOW, TAB, ROWS, OUT = 80, 640, 1280, 24, 2560, 3072

AX, BX, FX, AY, BY, FY, PO, PAX, PBX, PFX, PAY, PBY, PFY = range(13)
NX, NY, NC, ME, DG = 4, 2, 1, 0, 6
KINDS = (
    (NX, ME, ME, H), (NX, ME, H, H), (NX, NY, H, H),
    (NY, ME, H, H), (NY, ME, ME, H), (NY, NX, ME, H),
    (NC, ME, ME, T), (NC, NX, ME, H), (NC, NX, H, H), (NC, DG, H, H),
    (NC, NY, H, H), (NC, NY, ME, H), (NC, DG, ME, H),
)
TABLES = ((NX, ME), (NY, ME), (DG, ME), (NC, ME), (NC, NX), (NC, NY), (NC, DG))


def dot(a, b):
    return jnp.dot(a, b, preferred_element_type=F32)


def kernel(x, table, wg, wu, wd, y, xs, acc_g, acc_u, zo, pick, mix, w, tables,
           ag_s, ag_r, tb_s, tb_r, own_sem, wsem, a_s, a_r, sx_s, sy_s, t1_r, t2_r,
           cx_s, cy_s, rx_r, ry_r, ysem, ready, cred_p, cred_x, cred_y):
    chunks = x.shape[1] // CH
    me = lax.axis_index("ep")
    mx, my, mc = me // 4, (me // 2) % 2, me % 2

    def at(mask):
        px = 1 - mx if mask & 4 else mx
        py = 1 - my if mask & 2 else my
        pc = 1 - mc if mask & 1 else mc
        return 4 * px + 2 * py + pc

    def cols(c):
        return pl.ds(pl.multiple_of(c * CH, CH), CH)

    def rows(dev, first, n):
        return pl.ds(pl.multiple_of(dev * T + first, H), n)

    def to(mask):
        return {"ep": at(mask)}

    def ag_send(kind, c):
        link, owner, first, n = KINDS[kind]
        place = xs.at[c, rows(at(owner), first, n), :]
        src = x.at[pl.ds(first, n), cols(c)] if owner == 0 else place
        return pltpu.make_async_remote_copy(
            src_ref=src, dst_ref=place, send_sem=ag_s.at[kind, c], recv_sem=ag_r.at[kind, c],
            device_id=to(link), device_id_type=MESH)

    def ag_arrive(kind, c):
        link, owner, first, n = KINDS[kind]
        place = xs.at[c, rows(at(link ^ owner), first, n), :]
        pltpu.make_async_remote_copy(
            src_ref=place, dst_ref=place, send_sem=ag_s.at[kind, c], recv_sem=ag_r.at[kind, c],
            device_id=to(link), device_id_type=MESH).wait_recv()

    def start(c, *kinds):
        for kind in kinds:
            ag_send(kind, c).start()

    def arrive(c, *kinds):
        for kind in kinds:
            ag_arrive(kind, c)

    def tb_copy(i):
        link, owner = TABLES[i]
        src = table if owner == 0 else tables.at[at(owner)]
        return pltpu.make_async_remote_copy(
            src_ref=src, dst_ref=tables.at[at(owner)], send_sem=tb_s.at[i], recv_sem=tb_r.at[i],
            device_id=to(link), device_id_type=MESH)

    def tb_arrive(i):
        link, owner = TABLES[i]
        place = tables.at[at(link ^ owner)]
        pltpu.make_async_remote_copy(
            src_ref=place, dst_ref=place, send_sem=tb_s.at[i], recv_sem=tb_r.at[i],
            device_id=to(link), device_id_type=MESH).wait_recv()

    def w_first(g):
        c, e = g // 8, g % 8
        k = pl.ds(pl.multiple_of(c * CH, CH), CH)
        s = 2 * (g % 3)
        return (pltpu.make_async_copy(wg.at[e, k, :], w.at[s], wsem.at[s]),
                pltpu.make_async_copy(wu.at[e, k, :], w.at[s + 1], wsem.at[s + 1]))

    def w_second(q):
        d, e = q // 8, q % 8
        s = (q + 2) % NW
        for k in range(3):
            pltpu.make_async_copy(
                wd.at[e, pl.ds(k * CH, CH), cols(d)], w.at[s, :, pl.ds(k * CH, CH)], wsem.at[s]
            ).start()

    def w_second_wait(q):
        s = (q + 2) % NW
        pltpu.make_async_copy(wg.at[0, pl.ds(0, CH), :], w.at[s], wsem.at[s]).wait()

    barrier = pltpu.get_barrier_semaphore()
    for mask in (4, 2, 6, 1):
        pl.semaphore_signal(barrier, inc=1, device_id=to(mask), device_id_type=MESH)
    for g in range(3):
        for copy in w_first(g):
            copy.start()
    pl.semaphore_wait(barrier, 4)

    for i in range(4):
        tb_copy(i).start()
    start(0, AX, AY, BX, BY, PO)
    for c in range(chunks):
        pltpu.make_async_copy(x.at[:, cols(c)], xs.at[c, rows(me, 0, T), :], own_sem.at[c]).start()
    tables[me] = table[...]
    @pl.loop(0, 32)
    def _(i):
        r = pl.ds(pl.multiple_of(i * PAIR, PAIR), PAIR)
        acc_g[r, :] = jnp.zeros((PAIR, acc_g.shape[1]), F32)
        acc_u[r, :] = jnp.zeros((PAIR, acc_u.shape[1]), F32)

    for i in range(3):
        tb_arrive(i)
        tb_copy(i + 4).start()
    arrive(0, AX, AY)
    start(0, FX, FY, PAX, PAY)
    start(1, AX, AY, BX, BY, PO)
    start(2, AX, AY)
    for i in range(3, 7):
        tb_arrive(i)
    for i in range(7):
        tb_copy(i).wait_send()

    eye = jnp.where(
        lax.broadcasted_iota(jnp.int32, (T, T), 0) == lax.broadcasted_iota(jnp.int32, (T, T), 1),
        1.0, 0.0).astype(BF16)
    row40 = lax.broadcasted_iota(jnp.int32, (SL, T), 0).astype(F32)
    row48 = lax.broadcasted_iota(jnp.int32, (PAD, T), 0).astype(F32)

    @pl.loop(0, 8)
    def _(s):
        mine = (lax.broadcasted_iota(jnp.int32, (8, T), 0) + me * 8).astype(F32)
        slot = jnp.full((8, T), -1000.0, F32)
        gate = jnp.zeros((8, T), F32)
        for j in range(8):
            hit = tables[s, j:j + 1, :] == mine
            slot = jnp.where(hit, tables[s, 8 + j:9 + j, :], slot)
            gate = jnp.where(hit, tables[s, 16 + j:17 + j, :], gate)
        for e in range(0, 8, 2):
            pick[s, e * SL:e * SL + PAIR, :] = jnp.concatenate(
                [jnp.where(row40 == slot[i:i + 1, :], 1.0, 0.0) for i in (e, e + 1)], 0).astype(BF16)
        for e in range(8):
            zo[e * PAD:e * PAD + PAD, 0:T] = jnp.where(
                row48 == slot[e:e + 1, :], gate[e:e + 1, :], 0.0).astype(BF16)
        mix[s] = lax.dot_general(
            eye, zo[0:KP, 0:T], (((1,), (1,)), ((), ())), preferred_element_type=F32).astype(BF16)

    arrive(0, BX, BY)
    start(0, PBX, PBY)
    arrive(0, FX, FY)
    start(0, PFX, PFY)

    def gather(c):
        pltpu.make_async_copy(x.at[:, cols(c)], xs.at[c, rows(me, 0, T), :], own_sem.at[c]).wait()
        arrive(c, PO, PAX, PAY, PBX, PBY, PFX, PFY)

        for p in range(4):
            a = dot(pick[2 * p], xs[c, p * CH:p * CH + T, :])
            b = dot(pick[2 * p + 1], xs[c, p * CH + T:p * CH + CH, :])
            for e in range(8):
                zo[e * M + p * PAIR:e * M + p * PAIR + PAIR, :] = jnp.concatenate(
                    [a[e * SL:e * SL + SL], b[e * SL:e * SL + SL]], 0).astype(BF16)

    def of_expert(e):
        return pl.ds(e * M, M)

    @pl.loop(0, chunks - 1)
    def _(c):
        gather(c)
        for e in range(8):
            g = c * 8 + e
            for copy in w_first(g):
                copy.wait()
            s = 2 * (g % 3)
            r = of_expert(e)
            z = zo[r, :]
            for k in range(0, acc_g.shape[1], CH):
                kk = pl.ds(k, CH)
                acc_g[r, kk] += dot(z, w[s, :, kk])
                acc_u[r, kk] += dot(z, w[s + 1, :, kk])
            for copy in w_first(g + 3):
                copy.start()
            if e == 0:
                arrive(c + 1, AX, AY)
                start(c + 1, FX, FY, PAX, PAY)
            if e == 2:
                @pl.when(c + 2 < chunks)
                def _():
                    start(c + 2, BX, BY, PO)
            if e == 3:
                @pl.when(c + 3 < chunks)
                def _():
                    start(c + 3, AX, AY)
            if e == 4:
                arrive(c + 1, BX, BY)
                start(c + 1, PBX, PBY)
            if e == 6:
                arrive(c + 1, FX, FY)
                start(c + 1, PFX, PFY)

    gather(chunks - 1)

    @pl.loop(0, chunks)
    def _(c):
        for kind in range(13):
            ag_send(kind, c).wait_send()

    for mask in (4, 2, 1):
        pl.semaphore_signal(ready, inc=1, device_id=to(mask), device_id_type=MESH)

    def hidden(e, k):
        return xs.at[(e // 4) * 3 + k, pl.ds((e % 4) * M, M), :]

    for e in range(8):
        g = (chunks - 1) * 8 + e
        for copy in w_first(g):
            copy.wait()
        s = 2 * (g % 3)
        r = of_expert(e)
        z = zo[r, :]
        for k in range(3):
            kk = pl.ds(k * CH, CH)
            gg = acc_g[r, kk] + dot(z, w[s, :, kk])
            uu = acc_u[r, kk] + dot(z, w[s + 1, :, kk])
            hidden(e, k)[...] = (jax.nn.silu(gg) * uu).astype(BF16)
        if e < 5:
            for copy in w_first(g + 3):
                copy.start()
        else:
            w_second(2 * (e - 5))
            w_second(2 * (e - 5) + 1)

    pl.semaphore_wait(ready, 3)

    chip = 2 * mx + my
    chip_x, chip_y, chip_d = 2 * (1 - mx) + my, 2 * mx + 1 - my, 3 - chip

    def part(d, i, first, n):
        k = d % 4
        return acc_g.at[pl.ds(pl.multiple_of((k % 2) * 1024 + i * T + first, H), n),
                        pl.ds(pl.multiple_of((k // 2) * CH, CH), CH)]

    def got_a(d, i):
        return xs.at[6, pl.ds(pl.multiple_of((d % 2) * 1024 + i * T, T), T), :]

    def put_a(d, i):
        return xs.at[7, pl.ds(pl.multiple_of((d % 2) * 1024 + i * T, T), T), :]

    def got(d, first, n):
        return xs.at[d % 4, pl.ds(LOW + first, n), :]

    def put(d, first, n):
        return xs.at[4 + d % 2, pl.ds(LOW + first, n), :]

    def send_a(d, i):
        return pltpu.make_async_remote_copy(
            src_ref=put_a(d, i), dst_ref=got_a(d, i), send_sem=a_s.at[d % 2, i], recv_sem=a_r.at[d % 2, i],
            device_id=to(1), device_id_type=MESH)

    def send_x1(d):
        return pltpu.make_async_remote_copy(
            src_ref=put(d, 0, T), dst_ref=got(d, 0, T), send_sem=sx_s.at[d % 2], recv_sem=t1_r.at[d % 4],
            device_id=to(4), device_id_type=MESH)

    def send_y1(d):
        return pltpu.make_async_remote_copy(
            src_ref=put(d, T, T), dst_ref=got(d, T, T), send_sem=sy_s.at[d % 2], recv_sem=t2_r.at[d % 4],
            device_id=to(2), device_id_type=MESH)

    def send_y2(d):
        return pltpu.make_async_remote_copy(
            src_ref=put(d, CH, H), dst_ref=got(d, CH, H), send_sem=cy_s.at[d % 2], recv_sem=ry_r.at[d % 4],
            device_id=to(2), device_id_type=MESH)

    def send_x2(d):
        return pltpu.make_async_remote_copy(
            src_ref=put(d, PT, H), dst_ref=got(d, PT, H), send_sem=cx_s.at[d % 2], recv_sem=rx_r.at[d % 4],
            device_id=to(4), device_id_type=MESH)

    def send_out(d, n):
        return pltpu.make_async_copy(
            pick.at[2 * (d % 4) + n, pl.ds(0, T), :],
            y.at[:, pl.ds(pl.multiple_of(d * CH + n * T, T), T)], ysem.at[d % 4, n])

    def step_b(d):
        for i in range(4):
            send_a(d, i).wait_recv()

        @pl.when(d >= 2)
        def _():
            send_x1(d - 2).wait_send()
            send_y1(d - 2).wait_send()

        @pl.when(d >= 4)
        def _():
            pl.semaphore_wait(cred_x, 1)
            pl.semaphore_wait(cred_y, 1)

        def total(i, first):
            return part(d, i, first, H)[...] + got_a(d, i)[pl.ds(first, H), :].astype(F32)

        put(d, 0, H)[...] = total(chip_x, 0).astype(BF16)
        put(d, H, H)[...] = total(chip_d, 0).astype(BF16)
        send_x1(d).start()
        put(d, T, H)[...] = total(chip_y, H).astype(BF16)
        put(d, KP, H)[...] = total(chip_d, H).astype(BF16)
        send_y1(d).start()
        for i, first in ((chip, 0), (chip, H), (chip_y, 0), (chip_x, H)):
            part(d, i, first, H)[...] = total(i, first)

        @pl.when(d < chunks - 2)
        def _():
            pl.semaphore_signal(cred_p, inc=1, device_id=to(1), device_id_type=MESH)

    def step_c(d):
        @pl.when(d >= 2)
        def _():
            send_x2(d - 2).wait_send()
            send_y2(d - 2).wait_send()

        send_x1(d).wait_recv()
        put(d, CH, H)[...] = (part(d, chip_y, 0, H)[...] + got(d, H, H)[...].astype(F32)).astype(BF16)
        send_y2(d).start()
        send_y1(d).wait_recv()
        put(d, PT, H)[...] = (part(d, chip_x, H, H)[...] + got(d, KP, H)[...].astype(F32)).astype(BF16)
        send_x2(d).start()

    def step_d(d):
        @pl.when(d >= 4)
        def _():
            send_out(d - 4, 0).wait()
            send_out(d - 4, 1).wait()

        send_y2(d).wait_recv()
        top = part(d, chip, 0, H)[...] + got(d, 0, H)[...].astype(F32) + got(d, CH, H)[...].astype(F32)
        send_x2(d).wait_recv()
        low = part(d, chip, H, H)[...] + got(d, T, H)[...].astype(F32) + got(d, PT, H)[...].astype(F32)
        for n in range(2):
            pick[2 * (d % 4) + n, 0:H, :] = top[:, n * T:n * T + T].astype(BF16)
            pick[2 * (d % 4) + n, H:T, :] = low[:, n * T:n * T + T].astype(BF16)
            send_out(d, n).start()

        @pl.when(d < chunks - 4)
        def _():
            pl.semaphore_signal(cred_x, inc=1, device_id=to(4), device_id_type=MESH)
            pl.semaphore_signal(cred_y, inc=1, device_id=to(2), device_id_type=MESH)

    @pl.loop(0, chunks)
    def _(d):
        for e in range(0, 8, 2):
            q = d * 8 + e
            w_second_wait(q)
            w_second_wait(q + 1)
            for i in (e, e + 1):
                s = (d * 8 + i + 2) % NW
                out = dot(hidden(i, 0)[...], w[s, :, pl.ds(0, CH)])
                out += dot(hidden(i, 1)[...], w[s, :, pl.ds(CH, CH)])
                out += dot(hidden(i, 2)[...], w[s, :, pl.ds(1024, CH)])
                for p in range(8):
                    rows48 = out[p * SL:p * SL + PAD] if p < 7 else jnp.concatenate(
                        [out[p * SL:], jnp.zeros((8, CH), F32)], 0)
                    zo[p * KP + i * PAD:p * KP + i * PAD + PAD, :] = rows48.astype(BF16)
            if e == 0:
                w_second(q + NW)
                w_second(q + NW + 1)
            else:
                @pl.when(d < chunks - 1)
                def _():
                    w_second(q + NW)
                    w_second(q + NW + 1)
            if e == 2:
                @pl.when(d >= 1)
                def _():
                    step_b(d - 1)

        @pl.when(d >= 2)
        def _():
            pl.semaphore_wait(cred_p, 1)
            for i in range(4):
                send_a(d - 2, i).wait_send()

        for i in range(4):
            o = zo[pl.ds(pl.multiple_of((2 * i + 1 - mc) * KP, KP), KP), :]
            put_a(d, i)[...] = dot(mix[2 * i + 1 - mc], o).astype(BF16)
            send_a(d, i).start()
        for i in range(4):
            o = zo[pl.ds(pl.multiple_of((2 * i + mc) * KP, KP), KP), :]
            part(d, i, 0, T)[...] = dot(mix[2 * i + mc], o)

        @pl.when(d >= 2)
        def _():
            step_c(d - 2)

        @pl.when(d >= 3)
        def _():
            step_d(d - 3)

    last = chunks - 1
    step_b(last)
    step_c(last - 1)
    step_d(last - 2)
    step_c(last)
    step_d(last - 1)
    step_d(last)
    for d in (last - 1, last):
        for i in range(4):
            send_a(d, i).wait_send()
        for copy in (send_x1(d), send_y1(d), send_x2(d), send_y2(d)):
            copy.wait_send()
    for d in range(chunks - 4, chunks):
        for n in range(2):
            send_out(d, n).wait()


def solution(mesh):
    def body(x, expert, slot, gate, w_gate, w_up, w_down):
        tokens, dim = x.shape[2:]
        ff = w_gate.shape[2]
        slots = SL
        keep = slot[0, 0] < slots
        table = jnp.concatenate([
            expert[0, 0].astype(F32).T,
            jnp.where(keep, slot[0, 0], -1000).astype(F32).T,
            gate[0, 0].astype(BF16).astype(F32).T,
        ])
        dma = pltpu.SemaphoreType.DMA
        any_ = pl.BlockSpec(memory_space=pl.ANY)
        y = pl.pallas_call(
            kernel,
            out_shape=jax.ShapeDtypeStruct((tokens, dim), BF16),
            in_specs=[any_, pl.BlockSpec(memory_space=pltpu.VMEM), any_, any_, any_],
            out_specs=any_,
            scratch_shapes=[
                pltpu.VMEM((dim // CH, 8 * tokens, CH), BF16),
                pltpu.VMEM((ROWS, ff), F32),
                pltpu.VMEM((ROWS, ff), F32),
                pltpu.VMEM((OUT, CH), BF16),
                pltpu.VMEM((8, M, T), BF16),
                pltpu.VMEM((8, T, KP), BF16),
                pltpu.VMEM((NW, CH, ff), BF16),
                pltpu.VMEM((8, TAB, T), F32),
                dma((13, dim // CH)), dma((13, dim // CH)), dma((7,)), dma((7,)),
                dma((dim // CH,)), dma((NW,)),
                dma((2, 4)), dma((2, 4)), dma((2,)), dma((2,)), dma((4,)), dma((4,)),
                dma((2,)), dma((2,)), dma((4,)), dma((4,)), dma((4, 2)),
                pltpu.SemaphoreType.REGULAR, pltpu.SemaphoreType.REGULAR,
                pltpu.SemaphoreType.REGULAR, pltpu.SemaphoreType.REGULAR,
            ],
            compiler_params=pltpu.CompilerParams(
                collective_id=0, has_side_effects=True, vmem_limit_bytes=67043328),
        )(x[0, 0], table, w_gate, w_up, w_down)
        return y[None, None]

    tok = P("dp", "ep", None, None)
    wt = P("ep", None, None)
    return jax.shard_map(
        body, mesh=mesh, in_specs=(tok, tok, tok, tok, wt, wt, wt), out_specs=tok, check_vma=False
    )
```

```python
import functools

import jax
import jax.numpy as jnp
from jax import lax
from jax.experimental import pallas as pl
from jax.experimental.pallas import tpu as pltpu
from jax.sharding import PartitionSpec as P

MESH = pl.DeviceIdType.MESH
F32, BF16 = jnp.float32, jnp.bfloat16
CH = 512
NW = 6
H, T, M, SL, PAD, KP = 128, 256, 320, 40, 48, 384
PAIR, PT, LOW, TAB, ROWS, OUT = 80, 640, 1280, 24, 2560, 3072

AX, BX, FX, AY, BY, FY, PO, PAX, PBX, PFX, PAY, PBY, PFY = range(13)
NX, NY, NC, ME, DG = 4, 2, 1, 0, 6
KINDS = (
    (NX, ME, ME, H), (NX, ME, H, H), (NX, NY, H, H),
    (NY, ME, H, H), (NY, ME, ME, H), (NY, NX, ME, H),
    (NC, ME, ME, T), (NC, NX, ME, H), (NC, NX, H, H), (NC, DG, H, H),
    (NC, NY, H, H), (NC, NY, ME, H), (NC, DG, ME, H),
)
TABLES = ((NX, ME), (NY, ME), (DG, ME), (NC, ME), (NC, NX), (NC, NY), (NC, DG))


def dot(a, b):
    return jnp.dot(a, b, preferred_element_type=F32)


def kernel(x, expert, slot, gate, wg, wu, wd, y, xs, acc_g, acc_u, zo, pick, w, w2, tables,
           ag_s, ag_r, tb_s, tb_r, own_sem, mix_sem, wsem, a_s, a_r, sx_s, sy_s, t1_r, t2_r,
           cx_s, cy_s, rx_r, ry_r, ysem, ready, cred_p, cred_x, cred_y):
    last = x.shape[1] // CH
    me = lax.axis_index("ep")
    mx, my, mc = me // 4, (me // 2) % 2, me % 2

    def at(mask):
        px = 1 - mx if mask & 4 else mx
        py = 1 - my if mask & 2 else my
        pc = 1 - mc if mask & 1 else mc
        return 4 * px + 2 * py + pc

    def static(c):
        return isinstance(c, int)

    def wide(c):
        return T if static(c) and c in (0, last) else CH

    def cols(c):
        if static(c):
            return pl.ds(max(c * CH - T, 0), wide(c))
        return pl.ds(pl.multiple_of(c * CH - T, T), CH)

    def when(cond, fn):
        if isinstance(cond, bool):
            if cond:
                fn()
        else:
            pl.when(cond)(fn)

    def sized(c, fn, low=True):
        if static(c):
            if 0 <= c <= last:
                fn(c)
            return
        if low:
            when(c == 0, lambda: fn(0))
            when(c > 0, lambda: fn(c))
        else:
            when(c < last, lambda: fn(c))
            when(c == last, lambda: fn(last))

    def block(c, r):
        if static(c) and c == last:
            return xs.at[0, r, T:CH]
        return xs.at[c, r, 0:wide(c)]

    def rows(dev, first, n):
        return pl.ds(pl.multiple_of(dev * T + first, H), n)

    def to(mask):
        return {"ep": at(mask)}

    def ag_send(kind, c):
        link, owner, first, n = KINDS[kind]
        place = block(c, rows(at(owner), first, n))
        src = x.at[pl.ds(first, n), cols(c)] if owner == 0 else place
        return pltpu.make_async_remote_copy(
            src_ref=src, dst_ref=place, send_sem=ag_s.at[kind, c], recv_sem=ag_r.at[kind, c],
            device_id=to(link), device_id_type=MESH)

    def ag_arrive(kind, c):
        link, owner, first, n = KINDS[kind]
        place = block(c, rows(at(link ^ owner), first, n))
        pltpu.make_async_remote_copy(
            src_ref=place, dst_ref=place, send_sem=ag_s.at[kind, c], recv_sem=ag_r.at[kind, c],
            device_id=to(link), device_id_type=MESH).wait_recv()

    def start(c, *kinds):
        for kind in kinds:
            ag_send(kind, c).start()

    def arrive(c, *kinds):
        for kind in kinds:
            ag_arrive(kind, c)

    def tb_copy(i):
        link, owner = TABLES[i]
        src = tables.at[at(owner)]
        return pltpu.make_async_remote_copy(
            src_ref=src, dst_ref=tables.at[at(owner)], send_sem=tb_s.at[i], recv_sem=tb_r.at[i],
            device_id=to(link), device_id_type=MESH)

    def tb_arrive(i):
        link, owner = TABLES[i]
        place = tables.at[at(link ^ owner)]
        pltpu.make_async_remote_copy(
            src_ref=place, dst_ref=place, send_sem=tb_s.at[i], recv_sem=tb_r.at[i],
            device_id=to(link), device_id_type=MESH).wait_recv()

    def slot_of(s):
        return w.at[s] if s < NW else w2.at[s - NW]

    def w_first(c, e):
        s = 2 * (e % 4)
        k = pl.ds(0, wide(c))
        return [pltpu.make_async_copy(m.at[e, cols(c), :], slot_of(s + i).at[k, :], wsem.at[s + i])
                for i, m in enumerate((wg, wu))]

    def w_load(c, e):
        for copy in w_first(c, e):
            copy.start()

    def w_fetch(c, pair):
        w_load(c, 2 * pair)
        w_load(c, 2 * pair + 1)

    def w_next(c, e):
        if e < 4:
            w_load(c, e + 4)
        else:
            sized(c + 1, lambda n: w_load(n, e - 4), low=False)

    def w_wait(c, pair):
        for e in (2 * pair, 2 * pair + 1):
            for copy in w_first(c, e):
                copy.wait()

    def w_second(d, e):
        s = (d * 8 + e) % NW
        for k in range(0, wg.shape[2], CH):
            pltpu.make_async_copy(
                wd.at[e, pl.ds(k, CH), cols(d)], w.at[s, :, pl.ds(k, wide(d))], wsem.at[s]).start()

    def w_second_wait(d, e):
        s = (d * 8 + e) % NW
        part = pl.ds(0, wide(d))
        pltpu.make_async_copy(wg.at[0, part, :], w.at[s, part, :], wsem.at[s]).wait()
        return s

    tables[me, 0:8, :] = expert[...].astype(F32)
    tables[me, 8:16, :] = jnp.where(slot[...] < SL, slot[...], -1000).astype(F32)
    tables[me, 16:TAB, :] = gate[...].astype(BF16).astype(F32)
    barrier = pltpu.get_barrier_semaphore()
    for mask in (4, 2, 6, 1):
        pl.semaphore_signal(barrier, inc=1, device_id=to(mask), device_id_type=MESH)
    w_fetch(0, 0)
    w_fetch(0, 1)
    pl.semaphore_wait(barrier, 4)

    for i in range(4):
        tb_copy(i).start()
    start(0, AX, AY, BX, BY, PO)
    def own(c):
        return pltpu.make_async_copy(x.at[:, cols(c)], block(c, rows(me, 0, T)), own_sem.at[c])

    for c in range(last + 1):
        own(c).start()
    for i in range(3):
        tb_arrive(i)
        tb_copy(i + 4).start()
    arrive(0, AX, AY)
    start(0, FX, FY, PAX, PAY)
    start(1, AX, AY, BX, BY, PO)
    for i in range(3, 7):
        tb_arrive(i)
    for i in range(7):
        tb_copy(i).wait_send()

    eye = jnp.where(
        lax.broadcasted_iota(jnp.int32, (T, T), 0) == lax.broadcasted_iota(jnp.int32, (T, T), 1),
        1.0, 0.0).astype(BF16)
    row40 = lax.broadcasted_iota(jnp.int32, (SL, T), 0).astype(F32)
    row48 = lax.broadcasted_iota(jnp.int32, (PAD, T), 0).astype(F32)

    @pl.loop(0, 8)
    def _(s):
        mine = (lax.broadcasted_iota(jnp.int32, (8, T), 0) + me * 8).astype(F32)
        place = jnp.full((8, T), -1000.0, F32)
        share = jnp.zeros((8, T), F32)
        for j in range(8):
            hit = tables[s, j:j + 1, :] == mine
            place = jnp.where(hit, tables[s, 8 + j:9 + j, :], place)
            share = jnp.where(hit, tables[s, 16 + j:17 + j, :], share)
        for e in range(0, 8, 2):
            pick[s, e * SL:e * SL + PAIR, :] = jnp.concatenate(
                [jnp.where(row40 == place[i:i + 1, :], 1.0, 0.0) for i in (e, e + 1)], 0).astype(BF16)
        for e in range(8):
            zo[e * PAD:e * PAD + PAD, 0:T] = jnp.where(
                row48 == place[e:e + 1, :], share[e:e + 1, :], 0.0).astype(BF16)
        zo[pl.ds(pl.multiple_of(CH + s * T, T), T), 0:KP] = lax.dot_general(
            eye, zo[0:KP, 0:T], (((1,), (1,)), ((), ())), preferred_element_type=F32).astype(BF16)

    def mix_out(s):
        return pltpu.make_async_copy(
            zo.at[pl.ds(CH + s * T, T), pl.ds(0, KP)], y.at[:, pl.ds(s * KP, KP)], mix_sem.at[s])

    def mix_in(s):
        return pltpu.make_async_copy(
            y.at[:, pl.ds(s * KP, KP)],
            w2.at[1, pl.ds((s // 4) * T, T), pl.ds((s % 4) * KP, KP)], mix_sem.at[s])

    for s in range(8):
        mix_out(s).start()
    arrive(0, BX, BY)
    start(0, PBX, PBY)
    arrive(0, FX, FY)
    start(0, PFX, PFY)

    def gather(c):
        own(c).wait()
        arrive(c, PO, PAX, PAY, PBX, PBY, PFX, PFY)
        w_wait(c, 0)
        for p in range(4):
            a = dot(pick[2 * p], block(c, pl.ds(p * CH, T))[...])
            b = dot(pick[2 * p + 1], block(c, pl.ds(p * CH + T, T))[...])
            for e in range(8):
                zo[e * M + p * PAIR:e * M + p * PAIR + PAIR, 0:wide(c)] = jnp.concatenate(
                    [a[e * SL:e * SL + SL], b[e * SL:e * SL + SL]], 0).astype(BF16)

    for s in range(8):
        mix_out(s).wait()

    def pass_a(n):
        arrive(n, AX, AY)
        start(n, FX, FY, PAX, PAY)

    def pass_b(n):
        arrive(n, BX, BY)
        start(n, PBX, PBY)

    def pass_f(n):
        arrive(n, FX, FY)
        start(n, PFX, PFY)

    def of_expert(e):
        return pl.ds(e * M, M)

    def first(c):
        if not static(c):
            when(c > 1, lambda: sized(c + 1, pass_a, low=False))
        gather(c)
        k = pl.ds(0, wide(c))
        for pair in range(4):
            if pair:
                w_wait(c, pair)
            for e in (2 * pair, 2 * pair + 1):
                s = 2 * (e % 4)
                r = of_expert(e)
                z = zo[r, k]
                for n in range(0, acc_g.shape[1], CH):
                    nn = pl.ds(n, CH)
                    g = dot(z, slot_of(s)[k, nn])
                    u = dot(z, slot_of(s + 1)[k, nn])
                    if static(c):
                        acc_g[r, nn] = g
                        acc_u[r, nn] = u
                    else:
                        acc_g[r, nn] += g
                        acc_u[r, nn] += u
                w_next(c, e)
            if pair == 0 and static(c):
                pass_a(c + 1)
                start(c + 2, AX, AY)
            if pair == 0 and not static(c):
                @pl.when(c == 1)
                def _():
                    pass_a(2)
                    start(3, AX, AY)
            if pair == 1:
                sized(c + 2, lambda n: start(n, BX, BY, PO), low=False)
                if not static(c):
                    sized(c + 3, lambda n: start(n, AX, AY), low=False)
            if pair == (3 if static(c) else 2):
                sized(c + 1, pass_b, low=False)
                sized(c + 1, pass_f, low=False)

    first(0)
    pl.loop(1, last)(first)
    gather(last)

    def sent(c):
        for kind in range(13):
            ag_send(kind, c).wait_send()

    sent(0)
    pl.loop(1, last)(sent)
    sent(last)

    for mask in (4, 2, 1):
        pl.semaphore_signal(ready, inc=1, device_id=to(mask), device_id_type=MESH)

    def hidden(e, k):
        return xs.at[(e // 4) * 3 + k, pl.ds((e % 4) * M, M), :]

    for pair in range(4):
        if pair:
            w_wait(last, pair)
        for e in (2 * pair, 2 * pair + 1):
            s = 2 * (e % 4)
            r = of_expert(e)
            k = pl.ds(0, T)
            z = zo[r, k]
            for i in range(3):
                nn = pl.ds(i * CH, CH)
                g = acc_g[r, nn] + dot(z, slot_of(s)[k, nn])
                u = acc_u[r, nn] + dot(z, slot_of(s + 1)[k, nn])
                hidden(e, i)[...] = (jax.nn.silu(g) * u).astype(BF16)
        if pair < 2:
            w_fetch(last, pair + 2)
        else:
            for e in range(4 * pair - 8, min(4 * pair - 4, 6)):
                w_second(0, e)
    for s in range(8):
        mix_in(s).start()

    pl.semaphore_wait(ready, 3)

    chip = 2 * mx + my
    chip_x, chip_y, chip_d = 2 * (1 - mx) + my, 2 * mx + 1 - my, 3 - chip

    def part(d, i, first, n):
        k = d % 4
        r, c = (k % 2) * 2 * CH + i * T + first, (k // 2) * CH
        if not static(d):
            c = pl.multiple_of(c, CH)
        return acc_g.at[pl.ds(pl.multiple_of(r, H), n), pl.ds(c, wide(d))]

    def bank(slot, d, i):
        r = (d % 2) * 2 * CH + i * T
        if not (static(d) and static(i)):
            r = pl.multiple_of(r, T)
        return xs.at[slot, pl.ds(r, T), 0:wide(d)]

    def got_a(d, i):
        return bank(6, d, i)

    def put_a(d, i):
        return bank(7, d, i)

    def got(d, first, n):
        return xs.at[d % 4, pl.ds(LOW + first, n), 0:wide(d)]

    def put(d, first, n):
        return xs.at[4 + d % 2, pl.ds(LOW + first, n), 0:wide(d)]

    def send_a(d, i):
        return pltpu.make_async_remote_copy(
            src_ref=put_a(d, i), dst_ref=got_a(d, i), send_sem=a_s.at[d % 2, i], recv_sem=a_r.at[d % 2, i],
            device_id=to(1), device_id_type=MESH)

    def send_x1(d):
        return pltpu.make_async_remote_copy(
            src_ref=put(d, 0, T), dst_ref=got(d, 0, T), send_sem=sx_s.at[d % 2], recv_sem=t1_r.at[d % 4],
            device_id=to(4), device_id_type=MESH)

    def send_y1(d):
        return pltpu.make_async_remote_copy(
            src_ref=put(d, T, T), dst_ref=got(d, T, T), send_sem=sy_s.at[d % 2], recv_sem=t2_r.at[d % 4],
            device_id=to(2), device_id_type=MESH)

    def send_y2(d):
        return pltpu.make_async_remote_copy(
            src_ref=put(d, CH, H), dst_ref=got(d, CH, H), send_sem=cy_s.at[d % 2], recv_sem=ry_r.at[d % 4],
            device_id=to(2), device_id_type=MESH)

    def send_x2(d):
        return pltpu.make_async_remote_copy(
            src_ref=put(d, PT, H), dst_ref=got(d, PT, H), send_sem=cx_s.at[d % 2], recv_sem=rx_r.at[d % 4],
            device_id=to(4), device_id_type=MESH)

    def send_out(d):
        return [pltpu.make_async_copy(
            pick.at[2 * (d % 4) + n, pl.ds(0, T), :],
            y.at[:, pl.ds(cols(d).start + n * T, T)], ysem.at[d % 4, n])
            for n in range(wide(d) // T)]

    def step_b(d):
        for i in range(4):
            send_a(d, i).wait_recv()

        def free(n):
            send_x1(n).wait_send()
            send_y1(n).wait_send()

        def credit():
            pl.semaphore_wait(cred_x, 1)
            pl.semaphore_wait(cred_y, 1)

        if static(d):
            sized(d - 2, free)
        else:
            when(d == 2, lambda: free(0))
            when(d > 2, lambda: free(d - 2))
        when(d >= 4, credit)

        def total(i, first):
            return part(d, i, first, H)[...] + got_a(d, i)[pl.ds(first, H), :].astype(F32)

        put(d, 0, H)[...] = total(chip_x, 0).astype(BF16)
        put(d, H, H)[...] = total(chip_d, 0).astype(BF16)
        send_x1(d).start()
        put(d, T, H)[...] = total(chip_y, H).astype(BF16)
        put(d, KP, H)[...] = total(chip_d, H).astype(BF16)
        send_y1(d).start()
        for i, first in ((chip, 0), (chip, H), (chip_y, 0), (chip_x, H)):
            part(d, i, first, H)[...] = total(i, first)

        when(d < last - 1, lambda: pl.semaphore_signal(
            cred_p, inc=1, device_id=to(1), device_id_type=MESH))

    def step_c(d):
        def free(n):
            send_x2(n).wait_send()
            send_y2(n).wait_send()

        if static(d):
            sized(d - 2, free)
        else:
            when(d == 2, lambda: free(0))
            when(d > 2, lambda: free(d - 2))

        send_x1(d).wait_recv()
        put(d, CH, H)[...] = (part(d, chip_y, 0, H)[...] + got(d, H, H)[...].astype(F32)).astype(BF16)
        send_y2(d).start()
        send_y1(d).wait_recv()
        put(d, PT, H)[...] = (part(d, chip_x, H, H)[...] + got(d, KP, H)[...].astype(F32)).astype(BF16)
        send_x2(d).start()

    def step_d(d):
        def free(n):
            for copy in send_out(n):
                copy.wait()

        if static(d):
            sized(d - 4, free)
        else:
            when(d == 4, lambda: free(0))
            when(d > 4, lambda: free(d - 4))

        send_y2(d).wait_recv()
        top = part(d, chip, 0, H)[...] + got(d, 0, H)[...].astype(F32) + got(d, CH, H)[...].astype(F32)
        send_x2(d).wait_recv()
        low = part(d, chip, H, H)[...] + got(d, T, H)[...].astype(F32) + got(d, PT, H)[...].astype(F32)
        for n, copy in enumerate(send_out(d)):
            pick[2 * (d % 4) + n, 0:H, :] = top[:, n * T:n * T + T].astype(BF16)
            pick[2 * (d % 4) + n, H:T, :] = low[:, n * T:n * T + T].astype(BF16)
            copy.start()

        def give():
            pl.semaphore_signal(cred_x, inc=1, device_id=to(4), device_id_type=MESH)
            pl.semaphore_signal(cred_y, inc=1, device_id=to(2), device_id_type=MESH)

        when(d <= last - 4, give)

    def second(d):
        k = wide(d)
        for e in range(0, 8, 2):
            slots = [w_second_wait(d, e), w_second_wait(d, e + 1)]
            for i, s in zip((e, e + 1), slots):
                out = dot(hidden(i, 0)[...], w[s, :, pl.ds(0, k)])
                out += dot(hidden(i, 1)[...], w[s, :, pl.ds(CH, k)])
                out += dot(hidden(i, 2)[...], w[s, :, pl.ds(2 * CH, k)])
                for p in range(8):
                    piece = out[p * SL:p * SL + PAD] if p < 7 else jnp.concatenate(
                        [out[p * SL:], jnp.zeros((8, k), F32)], 0)
                    if p < 6:
                        zo[p * KP + i * PAD:p * KP + i * PAD + PAD, 0:k] = piece.astype(BF16)
                    else:
                        w2[0, i * PAD:i * PAD + PAD, pl.ds((p - 6) * CH, k)] = piece.astype(BF16)

            def more(n):
                for i in (e, e + 1):
                    w_second(n, (i + 6) % 8)
            if e == 0:
                more(d)
                sized(d - 1, step_b)
            else:
                sized(d + 1, more, low=False)

        def free(n):
            for i in range(4):
                send_a(n, i).wait_send()

        when(d >= 2, lambda: pl.semaphore_wait(cred_p, 1))
        if static(d):
            sized(d - 2, free)
        else:
            when(d == 2, lambda: free(0))
            when(d > 2, lambda: free(d - 2))

        if static(d) and d == 0:
            for s in range(8):
                mix_in(s).wait()

        def mixed(i, c):
            s = 2 * i + c
            mix = w2[1, pl.ds((i // 2) * T, T), pl.ds(pl.multiple_of((2 * (i % 2) + c) * KP, H), KP)]
            if i == 3:
                return dot(mix, w2[0, 0:KP, pl.ds(pl.multiple_of(c * CH, CH), k)])
            return dot(mix, zo[pl.ds(pl.multiple_of(s * KP, KP), KP), 0:k])

        for i in range(4):
            put_a(d, i)[...] = mixed(i, 1 - mc).astype(BF16)
            send_a(d, i).start()
        for i in range(4):
            part(d, i, 0, T)[...] = mixed(i, mc)

        if static(d):
            sized(d - 2, step_c)
            sized(d - 3, step_d)
        else:
            when(d == 2, lambda: step_c(0))
            when(d > 2, lambda: step_c(d - 2))
            when(d == 3, lambda: step_d(0))
            when(d > 3, lambda: step_d(d - 3))

    second(0)
    pl.loop(1, last)(second)
    second(last)
    step_b(last)
    step_c(last - 1)
    step_d(last - 2)
    step_c(last)
    step_d(last - 1)
    step_d(last)
    for d in (last - 1, last):
        for i in range(4):
            send_a(d, i).wait_send()
        for copy in (send_x1(d), send_y1(d), send_x2(d), send_y2(d)):
            copy.wait_send()
    for d in range(last - 3, last + 1):
        for copy in send_out(d):
            copy.wait()


def solution(mesh):
    def body(x, expert, slot, gate, w_gate, w_up, w_down):
        tokens, dim = x.shape[2:]
        ff = w_gate.shape[2]
        dma = pltpu.SemaphoreType.DMA
        any_ = pl.BlockSpec(memory_space=pl.ANY)
        y = pl.pallas_call(
            kernel,
            out_shape=jax.ShapeDtypeStruct((tokens, dim), BF16),
            in_specs=[any_] + [pl.BlockSpec(memory_space=pltpu.VMEM)] * 3 + [any_] * 3,
            out_specs=any_,
            scratch_shapes=[
                pltpu.VMEM((dim // CH, 8 * tokens, CH), BF16),
                pltpu.VMEM((ROWS, ff), F32),
                pltpu.VMEM((ROWS, ff), F32),
                pltpu.VMEM((ROWS, CH), BF16),
                pltpu.VMEM((8, M, T), BF16),
                pltpu.VMEM((NW, CH, ff), BF16),
                pltpu.VMEM((2, CH, ff), BF16),
                pltpu.VMEM((8, TAB, T), F32),
                dma((13, dim // CH + 1)), dma((13, dim // CH + 1)), dma((7,)), dma((7,)),
                dma((dim // CH + 1,)), dma((8,)), dma((NW + 2,)),
                dma((2, 4)), dma((2, 4)), dma((2,)), dma((2,)), dma((4,)), dma((4,)),
                dma((2,)), dma((2,)), dma((4,)), dma((4,)), dma((4, 2)),
                pltpu.SemaphoreType.REGULAR, pltpu.SemaphoreType.REGULAR,
                pltpu.SemaphoreType.REGULAR, pltpu.SemaphoreType.REGULAR,
            ],
            compiler_params=pltpu.CompilerParams(
                collective_id=0, has_side_effects=True, vmem_limit_bytes=67043328),
        )(x[0, 0], expert[0, 0].T, slot[0, 0].T, gate[0, 0].T, w_gate, w_up, w_down)
        return y[None, None]

    tok = P("dp", "ep", None, None)
    wt = P("ep", None, None)
    return jax.shard_map(
        body, mesh=mesh, in_specs=(tok, tok, tok, tok, wt, wt, wt), out_specs=tok, check_vma=False
    )
```
